64 devices in a mesh: dp: 4 (over x, y), sp: 16 (over z, core).
Axes of the slice: x: 2, y: 2, z: 8, core: 2. Of those that a mesh axis runs over, the one named last changes fastest.
The devices are a block of a 4x4x8 slice.
Arguments:
- x: bfloat16 [32768, 4096], P(('dp', 'sp')), parts along dimension 0
- doc_start: int32 [32768], P(('dp', 'sp')), parts along dimension 0
- w_in: bfloat16 [4096, 18560], replicated
- conv_w: float32 [4, 10240], replicated
- conv_b: float32 [10240], replicated
- dt_bias: float32 [128], replicated
- a_log: float32 [128], replicated
- d_skip: float32 [128], replicated
- norm_w: float32 [8, 1024], replicated
- w_out: bfloat16 [8192, 4096], replicated
Outputs:
- output: bfloat16 [32768, 4096], P(('dp', 'sp')), parts along dimension 0
There are 4 independent parts. The reference program is written for one: setup_inputs(seed, part) draws one part's arguments, and reference() takes and returns one part's arrays. A program takes and returns all parts, laid end to end along the dimension named above; an argument that names none is the same for every part.
All inputs are finite; a program needn't handle non-finite values.
Results may differ from the reference program's by a relative error of at most 0.00217803.
Values are sent between devices in bfloat16 or wider.
A program may use at most 768 MiB of HBM per device.

```python
import jax
import jax.numpy as jnp
from jax import lax

SEQ_LEN = 8192
SHARD_LEN = 512
D_MODEL = 4096
NUM_HEADS = 128
HEAD_DIM = 64
NUM_GROUPS = 8
STATE_DIM = 128
CHUNK_LEN = 256
CONV_WIDTH = 4
NORM_EPS = 1e-5
D_INNER = NUM_HEADS * HEAD_DIM
GROUP_WIDTH = D_INNER // NUM_GROUPS
PER_GROUP = NUM_HEADS // NUM_GROUPS
CONV_DIM = D_INNER + 2 * NUM_GROUPS * STATE_DIM
PROJ_DIM = 2 * D_INNER + 2 * NUM_GROUPS * STATE_DIM + NUM_HEADS
N_CHUNKS = SEQ_LEN // CHUNK_LEN
N_SHARDS = SEQ_LEN // SHARD_LEN


def draw_starts(start_key):
    level_key, pos_key = jax.random.split(start_key)
    shard_level = jax.random.randint(level_key, (N_SHARDS, 1), 0, 4)
    pos_draws = jax.random.randint(pos_key, (N_SHARDS, SHARD_LEN), 0, SHARD_LEN)
    return (pos_draws < shard_level).astype(jnp.int32).reshape(SEQ_LEN)


def setup_inputs(seed: int = 0, part: int = 0) -> dict:
    root_key = jax.random.key(seed)
    part_key = jax.random.fold_in(root_key, part)
    x_key, start_key = jax.random.split(part_key)
    weight_keys = jax.random.split(root_key, 8)
    x = jax.random.normal(x_key, (SEQ_LEN, D_MODEL), jnp.float32).astype(jnp.bfloat16)
    doc_start = draw_starts(start_key)
    w_in = (jax.random.normal(weight_keys[0], (D_MODEL, PROJ_DIM), jnp.float32) * D_MODEL ** -0.5).astype(jnp.bfloat16)
    conv_w = jax.random.normal(weight_keys[1], (CONV_WIDTH, CONV_DIM), jnp.float32) * 0.5
    conv_b = jax.random.normal(weight_keys[2], (CONV_DIM,), jnp.float32) * 0.5
    dt_bias = jax.random.uniform(weight_keys[3], (NUM_HEADS,), jnp.float32, -3.5, -2.5)
    decay_rate = jax.random.uniform(weight_keys[4], (NUM_HEADS,), jnp.float32, 0.3, 1.5)
    a_log = jnp.log(decay_rate) - jnp.log(0.08 * SHARD_LEN)
    d_skip = jax.random.uniform(weight_keys[5], (NUM_HEADS,), jnp.float32, 0.5, 1.5)
    norm_w = jax.random.uniform(weight_keys[6], (NUM_GROUPS, GROUP_WIDTH), jnp.float32, 0.5, 1.5)
    w_out = (jax.random.normal(weight_keys[7], (D_INNER, D_MODEL), jnp.float32) * D_INNER ** -0.5).astype(jnp.bfloat16)
    return {'x': x, 'doc_start': doc_start, 'w_in': w_in, 'conv_w': conv_w, 'conv_b': conv_b, 'dt_bias': dt_bias, 'a_log': a_log, 'd_skip': d_skip, 'norm_w': norm_w, 'w_out': w_out}


def chunk_step(run_state, chunk_in):
    xs_blk, b_blk, c_blk, dt_blk, ld_blk, start_blk = chunk_in
    cum_decay = jnp.cumsum(ld_blk, axis=0)
    seg_ids = jnp.cumsum(start_blk)
    position = jnp.arange(CHUNK_LEN)
    allowed = (position[:, None] >= position[None, :]) & (seg_ids[:, None] == seg_ids[None, :])
    cum_rows = jnp.moveaxis(cum_decay, 0, -1)
    decay_mat = jnp.exp(jnp.where(allowed, cum_rows[..., :, None] - cum_rows[..., None, :], -jnp.inf))
    scores = jnp.einsum('ign,jgn->gij', c_blk.astype(jnp.float32), b_blk.astype(jnp.float32))
    mix_mat = (scores[:, None] * decay_mat * jnp.moveaxis(dt_blk, 0, -1)[..., None, :]).astype(jnp.bfloat16)
    y_intra = jnp.einsum('gkij,jgkp->igkp', mix_mat.astype(jnp.float32), xs_blk.astype(jnp.float32))
    w_start = jnp.exp(cum_decay) * (seg_ids == 0)[:, None, None]
    y_state = jnp.einsum('ign,gkpn->igkp', c_blk.astype(jnp.float32), run_state.astype(jnp.bfloat16).astype(jnp.float32)) * w_start[..., None]
    last_cum = cum_decay[-1]
    w_end = jnp.exp(last_cum - cum_decay) * dt_blk * (seg_ids == seg_ids[-1])[:, None, None]
    scaled_x = (xs_blk.astype(jnp.float32) * w_end[..., None]).astype(jnp.bfloat16)
    chunk_state = jnp.einsum('jgkp,jgn->gkpn', scaled_x.astype(jnp.float32), b_blk.astype(jnp.float32))
    next_state = (jnp.exp(last_cum) * (seg_ids[-1] == 0))[..., None, None] * run_state + chunk_state
    return next_state, y_intra + y_state


def reference(x, doc_start, w_in, conv_w, conv_b, dt_bias, a_log, d_skip, norm_w, w_out):
    projected = jnp.dot(x, w_in, preferred_element_type=jnp.float32).astype(jnp.bfloat16)
    gate_in = projected[:, :D_INNER].astype(jnp.float32)
    conv_in = projected[:, D_INNER:D_INNER + CONV_DIM].astype(jnp.float32)
    dt_raw = projected[:, D_INNER + CONV_DIM:].astype(jnp.float32)
    keep_flag = (1 - doc_start).astype(jnp.float32)
    keep_pad = jnp.concatenate([jnp.ones((CONV_WIDTH - 1,), jnp.float32), keep_flag])
    conv_pad = jnp.concatenate([jnp.zeros((CONV_WIDTH - 1, CONV_DIM), jnp.float32), conv_in])
    pre_act = conv_b + conv_w[0] * conv_in
    tap_mask = jnp.ones((SEQ_LEN,), jnp.float32)
    for offset in range(1, CONV_WIDTH):
        tap_mask = tap_mask * keep_pad[CONV_WIDTH - offset:CONV_WIDTH - offset + SEQ_LEN]
        pre_act = pre_act + conv_w[offset] * tap_mask[:, None] * conv_pad[CONV_WIDTH - 1 - offset:CONV_WIDTH - 1 - offset + SEQ_LEN]
    conv_out = jax.nn.silu(pre_act).astype(jnp.bfloat16)
    xs_heads = conv_out[:, :D_INNER]
    b_mat = conv_out[:, D_INNER:D_INNER + NUM_GROUPS * STATE_DIM]
    c_mat = conv_out[:, D_INNER + NUM_GROUPS * STATE_DIM:]
    dt_val = jax.nn.softplus(dt_raw + dt_bias)
    log_decay = -jnp.exp(a_log) * dt_val
    chunk_inputs = (
        xs_heads.reshape(N_CHUNKS, CHUNK_LEN, NUM_GROUPS, PER_GROUP, HEAD_DIM),
        b_mat.reshape(N_CHUNKS, CHUNK_LEN, NUM_GROUPS, STATE_DIM),
        c_mat.reshape(N_CHUNKS, CHUNK_LEN, NUM_GROUPS, STATE_DIM),
        dt_val.reshape(N_CHUNKS, CHUNK_LEN, NUM_GROUPS, PER_GROUP),
        log_decay.reshape(N_CHUNKS, CHUNK_LEN, NUM_GROUPS, PER_GROUP),
        doc_start.reshape(N_CHUNKS, CHUNK_LEN),
    )
    zero_state = jnp.zeros((NUM_GROUPS, PER_GROUP, HEAD_DIM, STATE_DIM), jnp.float32)
    scan_out = lax.scan(chunk_step, zero_state, chunk_inputs)
    y_heads = scan_out[1].reshape(SEQ_LEN, NUM_HEADS, HEAD_DIM) + d_skip[:, None] * xs_heads.reshape(SEQ_LEN, NUM_HEADS, HEAD_DIM).astype(jnp.float32)
    gated_y = y_heads.reshape(SEQ_LEN, NUM_GROUPS, GROUP_WIDTH) * jax.nn.silu(gate_in).reshape(SEQ_LEN, NUM_GROUPS, GROUP_WIDTH)
    normed = gated_y * lax.rsqrt(jnp.mean(gated_y * gated_y, axis=-1, keepdims=True) + NORM_EPS) * norm_w
    return jnp.dot(normed.reshape(SEQ_LEN, D_INNER).astype(jnp.bfloat16), w_out, preferred_element_type=jnp.float32).astype(jnp.bfloat16)
```

```python
import functools
import jax
import jax.numpy as jnp
from jax import lax
from jax.experimental import pallas as pl
from jax.experimental.pallas import tpu as pltpu
from jax.sharding import PartitionSpec as P

CHUNK = 256
EPS = 1e-5
LOG2E = 1.4426950408889634
HALO = 16
COLS = 256
LAG = 3
VMEM = pltpu.VMEM
MESH = pl.DeviceIdType.MESH
F32 = jnp.float32
BF16 = jnp.bfloat16


def split3(v):
    hi = v.astype(BF16)
    rest = v - hi.astype(F32)
    mid = rest.astype(BF16)
    lo = (rest - mid.astype(F32)).astype(BF16)
    return hi, mid, lo


def dot(a, b):
    return jnp.dot(a, b, preferred_element_type=F32)


def dot_nt(a, b):
    return lax.dot_general(a, b, (((1,), (1,)), ((), ())), preferred_element_type=F32)


def prep_kernel(per, x_ref, w_ref, bias_ref, alog_ref, docc_ref, docr_ref, e_ref,
                aig_ref, ajt_ref, wst_ref, wend_ref, eexp_ref, dall_ref, mask_ref,
                tail_ref, segc_ref, segr_ref, keep_ref):
    n_tok = x_ref.shape[0]
    groups = aig_ref.shape[0]
    n_chunks = n_tok // CHUNK
    raw = dot(x_ref[...], w_ref[...]).astype(BF16).astype(F32) + bias_ref[...]
    dt = jnp.maximum(raw, 0.0) + jnp.log1p(jnp.exp(-jnp.abs(raw)))
    a = -jnp.exp(alog_ref[...]) * dt
    row = lax.broadcasted_iota(jnp.int32, (CHUNK, CHUNK), 0)
    col = lax.broadcasted_iota(jnp.int32, (CHUNK, CHUNK), 1)
    tri = (row >= col).astype(F32).astype(BF16)
    last_rows = []
    for c in range(n_chunks):
        rows = pl.ds(c * CHUNK, CHUNK)
        sl = slice(c * CHUNK, (c + 1) * CHUNK)
        hi, mid, lo = split3(a[sl])
        acum = dot(tri, hi) + (dot(tri, mid) + dot(tri, lo))
        dtc = dt[sl]
        segc = dot(tri, docc_ref[rows, :])
        segc_ref[rows, :] = segc
        segr_ref[:, rows] = dot_nt(docr_ref[:, rows], tri)
        a_last = acum[CHUNK - 1:CHUNK]
        s_last = segc[CHUNK - 1:CHUNK]
        wend = jnp.where(segc == s_last, jnp.exp(a_last - acum) * dtc, 0.0)
        wst = jnp.where(segc == 0.0, jnp.exp(acum), 0.0)
        e_c = jnp.where(s_last == 0.0, jnp.exp(a_last), 0.0)
        last_rows.append(e_c)
        ai = acum * LOG2E
        ajt_ref[:, rows] = (ai - jnp.log2(dtc)).T
        end3 = split3(wend)
        st3 = split3(wst)
        for g in range(groups):
            lanes = slice(g * per, (g + 1) * per)
            aig_ref[g, rows, :] = ai[:, lanes]
            wend_ref[g, rows, :] = jnp.concatenate([v[:, lanes] for v in end3], axis=1)
            wst_ref[g, rows, :] = jnp.concatenate([v[:, lanes] for v in st3], axis=1)
    total = last_rows[0]
    for e_c in last_rows[1:]:
        total = total * e_c
    n_row = len(last_rows)
    stack = jnp.concatenate(last_rows + [total] * (8 - n_row), axis=0)
    parts = split3(stack)
    for g in range(groups):
        lanes = slice(g * per, (g + 1) * per)
        cat = jnp.concatenate([v[:, lanes] for v in parts], axis=1)
        ex = dot(cat, e_ref[...])
        eexp_ref[g] = ex
        dall_ref[pl.ds(g, 1), :] = ex[n_row:n_row + 1]
    docf = docc_ref[...].astype(F32)
    keep_ref[pl.ds(0, 8), :] = jnp.ones((8, docf.shape[1]), F32)
    keep_ref[pl.ds(8, n_tok), :] = 1.0 - docf
    m1 = keep_ref[pl.ds(8, n_tok), :]
    m2 = m1 * keep_ref[pl.ds(7, n_tok), :]
    m3 = m2 * keep_ref[pl.ds(6, n_tok), :]
    mask_ref[0] = m1
    mask_ref[1] = m2
    mask_ref[2] = m3
    r16 = lax.broadcasted_iota(jnp.int32, (HALO, HALO), 0)
    c16 = lax.broadcasted_iota(jnp.int32, (HALO, HALO), 1)
    later = (c16 > r16).astype(F32).astype(BF16)
    cnt = dot(later, docc_ref[pl.ds(n_tok - HALO, HALO), :])
    tail = x_ref[pl.ds(n_tok - HALO, HALO), :].astype(F32)
    tail_ref[...] = jnp.where(cnt[:, :1] == 0.0, tail, 0.0).astype(BF16)


def proj_kernel(n_seq, groups, x_hbm, tail_ref, wa_ref, wbc_ref, cwx_ref, cwb_ref,
                mask_ref, wend_ref, eexp_ref, dall_ref, e_ref,
                xo_ref, bco_ref, z_ref, st0_ref, sin_hbm,
                xext, pbuf, btbuf, sloc, s1buf, rbuf, dpart,
                send_a, send_b, recv_s, recv_r, out_sem, misc):
    j = pl.program_id(0)
    idx = lax.axis_index('sp')
    core = lax.rem(idx, 2)
    chip = lax.div(idx, 2)
    n_chip = n_seq // 2
    n_tok = x_hbm.shape[0]
    n_chunks = n_tok // CHUNK
    n_q = wa_ref.shape[1] // COLS
    pieces = sloc.shape[0]
    halo_rows = pl.ds(0, HALO)

    def tail_copy(target):
        return pltpu.make_async_remote_copy(
            src_ref=tail_ref, dst_ref=xext.at[halo_rows], send_sem=misc.at[1], recv_sem=misc.at[2],
            device_id={'sp': target}, device_id_type=MESH)

    def decay_copy(target):
        return pltpu.make_async_remote_copy(
            src_ref=dall_ref, dst_ref=dpart, send_sem=misc.at[3], recv_sem=misc.at[4],
            device_id={'sp': target}, device_id_type=MESH)

    def state_copy(p, target):
        return pltpu.make_async_remote_copy(
            src_ref=sloc.at[p], dst_ref=s1buf.at[p], send_sem=send_a.at[p], recv_sem=recv_s.at[p],
            device_id={'sp': target}, device_id_type=MESH)

    def entry_copy(p, target):
        return pltpu.make_async_remote_copy(
            src_ref=sloc.at[p], dst_ref=rbuf.at[p], send_sem=send_a.at[p], recv_sem=recv_r.at[p],
            device_id={'sp': target}, device_id_type=MESH)

    def chain_copy(p, target):
        return pltpu.make_async_remote_copy(
            src_ref=s1buf.at[p], dst_ref=rbuf.at[p], send_sem=send_b.at[p], recv_sem=recv_r.at[p],
            device_id={'sp': target}, device_id_type=MESH)

    def out_copy(p):
        return pltpu.make_async_copy(rbuf.at[p], sin_hbm.at[p], out_sem.at[p])

    @pl.when(j == 0)
    def _():
        own = pltpu.make_async_copy(x_hbm, xext.at[pl.ds(HALO, n_tok)], misc.at[0])
        own.start()
        barrier = pltpu.get_barrier_semaphore()
        links = [(idx > 0, idx - 1), (idx < n_seq - 1, idx + 1),
                 ((core == 0) & (idx > 1), idx - 2), ((core == 0) & (idx < n_seq - 2), idx + 2)]
        for ok, other in links:
            @pl.when(ok)
            def _(other=other):
                pl.semaphore_signal(barrier, inc=1, device_id={'sp': other}, device_id_type=MESH)
        pl.semaphore_wait(barrier, sum(ok.astype(jnp.int32) for ok, other in links))

        @pl.when(idx < n_seq - 1)
        def _():
            tail_copy(idx + 1).start()

        @pl.when(core == 1)
        def _():
            decay_copy(idx - 1).start()

        @pl.when(idx == 0)
        def _():
            xext[halo_rows, :] = jnp.zeros((HALO, xext.shape[1]), BF16)

            def clear(p, carry):
                rbuf[p] = jnp.zeros(rbuf.shape[1:], F32)
                return carry
            lax.fori_loop(0, pieces, clear, 0)

        @pl.when(idx > 0)
        def _():
            tail_copy(idx).wait_recv()
        own.wait()

    def tick(t):
        @pl.when((core == 1) & (t < pieces))
        def _():
            state_copy(t, idx - 1).start()

        p = t - 1 - LAG * chip

        @pl.when((core == 0) & (p >= 0) & (p < pieces))
        def _():
            @pl.when(p == 0)
            def _():
                decay_copy(idx).wait_recv()
            state_copy(p, idx).wait_recv()

            @pl.when(chip > 0)
            def _():
                entry_copy(p, idx).wait_recv()
            grp = lax.div(p, n_q)
            lanes = pl.ds(pl.multiple_of(lax.rem(p, n_q) * COLS, COLS), COLS)
            d_own = dall_ref[pl.ds(grp, 1), lanes]
            d_par = dpart[pl.ds(grp, 1), lanes]
            mid = d_own * rbuf[p] + sloc[p]
            sloc[p] = mid
            s1buf[p] = d_par * mid + s1buf[p]

            @pl.when(chip < n_chip - 1)
            def _():
                chain_copy(p, idx + 2).start()
            entry_copy(p, idx + 1).start()
            out_copy(p).start()

        r = p - 2

        @pl.when((core == 1) & (r >= 0) & (r < pieces))
        def _():
            entry_copy(r, idx).wait_recv()
            out_copy(r).start()

    def conv(slot, cw_ref, lanes):
        buf = pbuf.at[slot]
        acc = cw_ref[4:5, lanes] + cw_ref[0:1, lanes] * buf[pl.ds(HALO, n_tok), :]
        for k in range(1, 4):
            m = mask_ref[k - 1]
            m = jnp.concatenate([m] * (COLS // m.shape[1]), axis=1)
            acc = acc + cw_ref[k:k + 1, lanes] * (m * buf[pl.ds(HALO - k, n_tok), :])
        half = 0.5 * acc
        return (half + half * jnp.tanh(half)).astype(BF16)

    def project(w, slot):
        pbuf[slot] = dot(xext[...], w).astype(BF16).astype(F32)

    @pl.when(j < groups)
    def _():
        par = lax.rem(j, 2)

        def epi_bc(slot):
            v = conv(slot, cwb_ref, slice(0, COLS))
            bco_ref[...] = v
            half = COLS // 2
            vt = v.T
            btbuf[2 * par] = vt[:half]
            btbuf[2 * par + 1] = vt[half:]

        def epi_x(q, slot):
            lanes = slice(q * COLS, (q + 1) * COLS)
            v = conv(slot, cwx_ref, lanes)
            xo_ref[:, lanes] = v
            wexp = dot(wend_ref[0], e_ref[:, lanes])
            xs = (v.astype(F32) * wexp).astype(BF16)
            tot = None
            for c in range(n_chunks):
                st = dot(btbuf[par, :, c * CHUNK:(c + 1) * CHUNK], xs[c * CHUNK:(c + 1) * CHUNK])
                if c == 0:
                    st0_ref[0, :, lanes] = st
                    tot = st
                else:
                    tot = eexp_ref[0, c:c + 1, lanes] * tot + st
            sloc[j * n_q + q] = tot

        project(wbc_ref[...], 0)
        for q in range(n_q):
            project(wa_ref[:, q * COLS:(q + 1) * COLS], (q + 1) % 2)
            if q == 0:
                epi_bc(0)
            else:
                epi_x(q - 1, q % 2)
                tick(j * n_q + q - 1)
        epi_x(n_q - 1, n_q % 2)
        tick(j * n_q + n_q - 1)

    @pl.when(j >= groups)
    def _():
        for q in range(n_q):
            lanes = slice(q * COLS, (q + 1) * COLS)
            z_ref[:, lanes] = dot(xext[pl.ds(HALO, n_tok), :], wa_ref[:, lanes]).astype(BF16)
            tick(j * n_q + q)

    @pl.when(j == 2 * groups - 1)
    def _():
        @pl.when(idx < n_seq - 1)
        def _():
            tail_copy(idx).wait_send()

        @pl.when(core == 1)
        def _():
            decay_copy(idx).wait_send()

        def drain(p, carry):
            state_copy(p, idx).wait_send()

            @pl.when((core == 0) & (chip < n_chip - 1))
            def _():
                chain_copy(p, idx).wait_send()
            out_copy(p).wait()
            return carry
        lax.fori_loop(0, pieces, drain, 0)


def mix_kernel(per, head, x_ref, z_ref, b_ref, c_ref, aig_ref, ajt_ref, wst_ref, segc_ref, segr_ref,
               sin_ref, st0_ref, eexp_ref, e_ref, skip_ref, norm_ref, o_ref, sc_ref, g_ref):
    n_tok, width = x_ref.shape
    n_chunks = n_tok // CHUNK
    half = CHUNK // 2
    pair = 2 * head
    row = lax.broadcasted_iota(jnp.int32, (CHUNK, CHUNK), 0)
    col = lax.broadcasted_iota(jnp.int32, (CHUNK, CHUNK), 1)
    first = lax.broadcasted_iota(jnp.int32, (half, pair), 1) < head
    n_piece = sin_ref.shape[0]
    pw = sin_ref.shape[2]
    for c in range(n_chunks):
        rows = slice(c * CHUNK, (c + 1) * CHUNK)
        cc = c_ref[rows, :]
        raw = dot_nt(cc, b_ref[rows, :])
        sc = segc_ref[rows, :]
        sc = jnp.concatenate([sc] * (CHUNK // sc.shape[1]), axis=1)
        same = sc == segr_ref[0:1, rows]
        sc_ref[...] = jnp.where(same & (row >= col), raw, 0.0)
        wst = wst_ref[0, rows, :]
        for k in range(n_piece):
            lanes = slice(k * pw, (k + 1) * pw)
            state = sin_ref[k]
            if c > 0:
                state = eexp_ref[0, 0:1, lanes] * state + st0_ref[0, :, lanes]
            ys = dot(cc, state.astype(BF16)) * dot(wst, e_ref[:, lanes])
            g_ref[:, lanes] = ys + skip_ref[0, :, lanes] * x_ref[rows, lanes].astype(F32)
        for hp in range(per // 2):
            lanes = slice(hp * pair, (hp + 1) * pair)
            xp = x_ref[rows, lanes]
            tops, bots = [], []
            for hh in range(2):
                h = 2 * hp + hh
                aj = ajt_ref[h:h + 1, rows]
                ai_t = aig_ref[0, c * CHUNK:c * CHUNK + half, h:h + 1]
                ai_b = aig_ref[0, c * CHUNK + half:(c + 1) * CHUNK, h:h + 1]
                m_tt = sc_ref[0:half, 0:half] * jnp.exp2(jnp.minimum(ai_t - aj[:, 0:half], 127.99))
                m_bl = sc_ref[half:CHUNK, 0:half] * jnp.exp2(jnp.minimum(ai_b - aj[:, 0:half], 127.99))
                m_br = sc_ref[half:CHUNK, half:CHUNK] * jnp.exp2(jnp.minimum(ai_b - aj[:, half:CHUNK], 127.99))
                tops.append(dot(m_tt.astype(BF16), xp[0:half]))
                m_b = jnp.concatenate([m_bl.astype(BF16), m_br.astype(BF16)], axis=1)
                bots.append(dot(m_b, xp))
            g_ref[0:half, lanes] += jnp.where(first, tops[0], tops[1])
            g_ref[half:CHUNK, lanes] += jnp.where(first, bots[0], bots[1])
        zf = z_ref[rows, :].astype(F32)
        hz = 0.5 * zf
        gated = g_ref[...] * (hz + hz * jnp.tanh(hz))
        mean = jnp.sum(gated * gated, axis=1, keepdims=True) * (1.0 / width)
        o_ref[rows, :] = (gated * lax.rsqrt(mean + EPS) * norm_ref[0]).astype(BF16)


def out_kernel(g_ref, w_ref, o_ref):
    o_ref[...] = dot(g_ref[...], w_ref[...]).astype(BF16)


def solution(mesh):
    n_seq = mesh.shape['sp']
    row_spec = P(('dp', 'sp'), None)
    tok_spec = P(('dp', 'sp'))

    def layer_shard(x, doc_start, w_in, conv_w, conv_b, dt_bias, a_log, d_skip, norm_w, w_out):
        n_tok, d_model = x.shape
        groups, gw = norm_w.shape
        d_inner = groups * gw
        n_heads = a_log.shape[0]
        per = n_heads // groups
        head = d_inner // n_heads
        conv_dim = conv_w.shape[1]
        sdim = (conv_dim - d_inner) // (2 * groups)
        n_q = gw // COLS
        pieces = groups * n_q
        lim = 67043328

        lane_head = jnp.arange(gw) // head
        expand = (lane_head[None, :] == jnp.arange(per)[:, None])
        expand = jnp.concatenate([expand] * 3, axis=0).astype(BF16)
        docf = doc_start.astype(BF16)
        docc = jnp.broadcast_to(docf[:, None], (n_tok, 128))
        docr = jnp.broadcast_to(docf[None, :], (8, n_tok))
        cw = jnp.concatenate([conv_w, conv_b[None], jnp.zeros((3, conv_dim), F32)], axis=0)
        skip = jnp.repeat(d_skip, head).reshape(groups, 1, gw)

        sds = jax.ShapeDtypeStruct
        full = lambda *shape: pl.BlockSpec(shape, lambda i: (0,) * len(shape))
        k3 = 3 * per
        dt_block = (d_inner + conv_dim) // n_heads
        prep = pl.pallas_call(
            functools.partial(prep_kernel, per),
            grid=(1,),
            in_specs=[full(n_tok, d_model), pl.BlockSpec((d_model, n_heads), lambda i: (0, dt_block)),
                      full(1, n_heads), full(1, n_heads), full(n_tok, 128), full(8, n_tok), full(k3, gw)],
            out_specs=[full(groups, n_tok, per), full(n_heads, n_tok), full(groups, n_tok, k3), full(groups, n_tok, k3),
                       full(groups, 8, gw), full(groups, gw), full(3, n_tok, 128), full(HALO, d_model),
                       full(n_tok, 128), full(8, n_tok)],
            out_shape=[sds((groups, n_tok, per), F32), sds((n_heads, n_tok), F32), sds((groups, n_tok, k3), BF16),
                       sds((groups, n_tok, k3), BF16), sds((groups, 8, gw), F32), sds((groups, gw), F32),
                       sds((3, n_tok, 128), F32), sds((HALO, d_model), BF16), sds((n_tok, 128), F32), sds((8, n_tok), F32)],
            scratch_shapes=[VMEM((n_tok + 8, 128), F32)],
            compiler_params=pltpu.CompilerParams(vmem_limit_bytes=lim),
            name='prep',
        )
        aig, ajt, wst3, wend3, eexp, dall, masks, tail, segc, segr = prep(
            x, w_in, dt_bias[None], a_log[None], docc, docr, expand)

        cap = lambda i: jnp.minimum(i, groups - 1)
        z_of = lambda i: jnp.maximum(i - groups, 0)
        pairs = groups // 2
        bc_of = lambda i: lax.rem(cap(i), 2) * pairs + lax.div(cap(i), 2)
        x_blk = d_inner // gw
        bc_blk = 2 * d_inner // COLS
        cb_blk = d_inner // COLS
        proj = pl.pallas_call(
            functools.partial(proj_kernel, n_seq, groups),
            grid=(2 * groups,),
            in_specs=[pl.BlockSpec(memory_space=pl.ANY), full(HALO, d_model),
                      pl.BlockSpec((d_model, gw), lambda i: (0, jnp.where(i < groups, i + x_blk, i - groups))),
                      pl.BlockSpec((d_model, COLS), lambda i: (0, bc_blk + bc_of(i))),
                      pl.BlockSpec((8, gw), lambda i: (0, cap(i))),
                      pl.BlockSpec((8, COLS), lambda i: (0, cb_blk + bc_of(i))),
                      full(3, n_tok, 128),
                      pl.BlockSpec((1, n_tok, k3), lambda i: (cap(i), 0, 0)),
                      pl.BlockSpec((1, 8, gw), lambda i: (cap(i), 0, 0)),
                      full(groups, gw), full(k3, gw)],
            out_specs=[pl.BlockSpec((n_tok, gw), lambda i: (0, cap(i))),
                       pl.BlockSpec((n_tok, COLS), lambda i: (0, bc_of(i))),
                       pl.BlockSpec((n_tok, gw), lambda i: (0, z_of(i))),
                       pl.BlockSpec((1, sdim, gw), lambda i: (cap(i), 0, 0)),
                       pl.BlockSpec(memory_space=pl.ANY)],
            out_shape=[sds((n_tok, d_inner), BF16), sds((n_tok, conv_dim - d_inner), BF16), sds((n_tok, d_inner), BF16),
                       sds((groups, sdim, gw), F32), sds((pieces, sdim, COLS), F32)],
            scratch_shapes=[VMEM((n_tok + HALO, d_model), BF16), VMEM((2, n_tok + HALO, COLS), F32),
                            VMEM((4, sdim, n_tok), BF16), VMEM((pieces, sdim, COLS), F32),
                            VMEM((pieces, sdim, COLS), F32), VMEM((pieces, sdim, COLS), F32), VMEM((groups, gw), F32),
                            pltpu.SemaphoreType.DMA((pieces,)), pltpu.SemaphoreType.DMA((pieces,)),
                            pltpu.SemaphoreType.DMA((pieces,)), pltpu.SemaphoreType.DMA((pieces,)),
                            pltpu.SemaphoreType.DMA((pieces,)), pltpu.SemaphoreType.DMA((5,))],
            compiler_params=pltpu.CompilerParams(vmem_limit_bytes=lim, collective_id=0, has_side_effects=True),
            name='proj',
        )
        xc, bc, z, st0, s_in = proj(x, tail, w_in, w_in, cw, cw, masks, wend3, eexp, dall, expand)

        mix = pl.pallas_call(
            functools.partial(mix_kernel, per, head),
            grid=(groups,),
            in_specs=[pl.BlockSpec((n_tok, gw), lambda i: (0, i)), pl.BlockSpec((n_tok, gw), lambda i: (0, i)),
                      pl.BlockSpec((n_tok, sdim), lambda i: (0, i)), pl.BlockSpec((n_tok, sdim), lambda i: (0, groups + i)),
                      pl.BlockSpec((1, n_tok, per), lambda i: (i, 0, 0)), pl.BlockSpec((per, n_tok), lambda i: (i, 0)),
                      pl.BlockSpec((1, n_tok, k3), lambda i: (i, 0, 0)), full(n_tok, 128), full(8, n_tok),
                      pl.BlockSpec((n_q, sdim, COLS), lambda i: (i, 0, 0)), pl.BlockSpec((1, sdim, gw), lambda i: (i, 0, 0)),
                      pl.BlockSpec((1, 8, gw), lambda i: (i, 0, 0)), full(k3, gw),
                      pl.BlockSpec((1, 1, gw), lambda i: (i, 0, 0)), pl.BlockSpec((1, 1, gw), lambda i: (i, 0, 0))],
            out_specs=pl.BlockSpec((n_tok, gw), lambda i: (0, i)),
            out_shape=sds((n_tok, d_inner), BF16),
            scratch_shapes=[VMEM((CHUNK, CHUNK), F32), VMEM((CHUNK, gw), F32)],
            compiler_params=pltpu.CompilerParams(vmem_limit_bytes=lim),
            name='mix',
        )
        g = mix(xc, z, bc, bc, aig, ajt, wst3, segc, segr, s_in, st0, eexp, expand, skip, norm_w[:, None, :])

        out_cols = 512
        out = pl.pallas_call(
            out_kernel,
            grid=(d_model // out_cols,),
            in_specs=[full(n_tok, d_inner), pl.BlockSpec((d_inner, out_cols), lambda i: (0, i))],
            out_specs=pl.BlockSpec((n_tok, out_cols), lambda i: (0, i)),
            out_shape=sds((n_tok, d_model), BF16),
            compiler_params=pltpu.CompilerParams(vmem_limit_bytes=lim),
            name='outproj',
        )
        return out(g, w_out)

    return jax.shard_map(layer_shard, mesh=mesh, in_specs=(row_spec, tok_spec, P(), P(), P(), P(), P(), P(), P(), P()), out_specs=row_spec, check_vma=False)
```

```python
import functools
import jax
import jax.numpy as jnp
from jax import lax
from jax.experimental import pallas as pl
from jax.experimental.pallas import tpu as pltpu
from jax.sharding import PartitionSpec as P

CHUNK = 256
EPS = 1e-5
LOG2E = 1.4426950408889634
HALO = 16
COLS = 256
LAG = 3
VMEM = pltpu.VMEM
MESH = pl.DeviceIdType.MESH
F32 = jnp.float32
BF16 = jnp.bfloat16


def split3(v):
    hi = v.astype(BF16)
    rest = v - hi.astype(F32)
    mid = rest.astype(BF16)
    lo = (rest - mid.astype(F32)).astype(BF16)
    return hi, mid, lo


def dot(a, b):
    return jnp.dot(a, b, preferred_element_type=F32)


def dot_nt(a, b):
    return lax.dot_general(a, b, (((1,), (1,)), ((), ())), preferred_element_type=F32)


def prep_kernel(per, head, x_ref, w_ref, bias_ref, alog_ref, skip_ref, doc_ref,
                ai_ref, ajt_ref, wst_ref, wend_ref, eexp_ref, dall_ref, mask_ref,
                tail_ref, segc_ref, segr_ref, e_ref, keep_ref):
    n_tok = x_ref.shape[0]
    doc = doc_ref[...].astype(F32)
    docr = jnp.broadcast_to(doc, (8, n_tok)).astype(BF16)
    docf = jnp.broadcast_to(doc, (128, n_tok)).T
    docc = docf.astype(BF16)
    e_row = lax.rem(lax.broadcasted_iota(jnp.int32, e_ref.shape, 0), per)
    e_col = lax.div(lax.broadcasted_iota(jnp.int32, e_ref.shape, 1), head)
    expand = (e_row == e_col).astype(F32).astype(BF16)
    e_ref[...] = expand
    groups = wst_ref.shape[0]
    n_chunks = n_tok // CHUNK
    raw = dot(x_ref[...], w_ref[...]).astype(BF16).astype(F32) + bias_ref[...]
    dt = jnp.maximum(raw, 0.0) + jnp.log1p(jnp.exp(-jnp.abs(raw)))
    a = -jnp.exp(alog_ref[...]) * dt
    row = lax.broadcasted_iota(jnp.int32, (CHUNK, CHUNK), 0)
    col = lax.broadcasted_iota(jnp.int32, (CHUNK, CHUNK), 1)
    tri = (row >= col).astype(F32).astype(BF16)
    last_rows = []
    for c in range(n_chunks):
        rows = pl.ds(c * CHUNK, CHUNK)
        sl = slice(c * CHUNK, (c + 1) * CHUNK)
        hi, mid, lo = split3(a[sl])
        acum = dot(tri, hi) + (dot(tri, mid) + dot(tri, lo))
        dtc = dt[sl]
        segc = dot(tri, docc[sl])
        segc_ref[rows, :] = segc
        segr_ref[:, rows] = dot_nt(docr[:, sl], tri)
        a_last = acum[CHUNK - 1:CHUNK]
        s_last = segc[CHUNK - 1:CHUNK]
        wend = jnp.where(segc == s_last, jnp.exp(a_last - acum) * dtc, 0.0)
        wst = jnp.where(segc == 0.0, jnp.exp(acum), 0.0)
        e_c = jnp.where(s_last == 0.0, jnp.exp(a_last), 0.0)
        last_rows.append(e_c)
        ai = acum * LOG2E
        ai_ref[rows, :] = ai
        ajt_ref[:, rows] = (ai - jnp.log2(dtc)).T
        end3 = split3(wend)
        st3 = split3(wst)
        for g in range(groups):
            lanes = slice(g * per, (g + 1) * per)
            wend_ref[g, rows, :] = jnp.concatenate([v[:, lanes] for v in end3], axis=1)
            wst_ref[g, rows, :] = jnp.concatenate([v[:, lanes] for v in st3], axis=1)
    total = last_rows[0]
    for e_c in last_rows[1:]:
        total = total * e_c
    n_row = len(last_rows)
    stack = jnp.concatenate(last_rows + [total] * (7 - n_row) + [skip_ref[...]], axis=0)
    parts = split3(stack)
    for g in range(groups):
        lanes = slice(g * per, (g + 1) * per)
        cat = jnp.concatenate([v[:, lanes] for v in parts], axis=1)
        ex = dot(cat, expand)
        eexp_ref[g] = ex
        dall_ref[pl.ds(g, 1), :] = ex[n_row:n_row + 1]
    keep_ref[pl.ds(0, 8), :] = jnp.ones((8, docf.shape[1]), F32)
    keep_ref[pl.ds(8, n_tok), :] = 1.0 - docf
    m1 = keep_ref[pl.ds(8, n_tok), :]
    m2 = m1 * keep_ref[pl.ds(7, n_tok), :]
    m3 = m2 * keep_ref[pl.ds(6, n_tok), :]
    mask_ref[0] = m1
    mask_ref[1] = m2
    mask_ref[2] = m3
    r16 = lax.broadcasted_iota(jnp.int32, (HALO, HALO), 0)
    c16 = lax.broadcasted_iota(jnp.int32, (HALO, HALO), 1)
    later = (c16 > r16).astype(F32).astype(BF16)
    cnt = dot(later, docc[n_tok - HALO:])
    tail = x_ref[pl.ds(n_tok - HALO, HALO), :].astype(F32)
    tail_ref[...] = jnp.where(cnt[:, :1] == 0.0, tail, 0.0).astype(BF16)


def proj_kernel(n_seq, groups, x_hbm, tail_ref, wa_ref, wbc_ref, cwx_ref, cbx_ref, cwb_ref, cbb_ref,
                mask_ref, wend_ref, eexp_ref, dall_ref, e_ref,
                xo_ref, bco_ref, z_ref, st0_ref, sin_hbm,
                xext, pbuf, btbuf, sloc, s1buf, rbuf, dpart,
                send_a, send_b, recv_s, recv_r, out_sem, misc):
    j = pl.program_id(0)
    idx = lax.axis_index('sp')
    core = lax.rem(idx, 2)
    chip = lax.div(idx, 2)
    n_chip = n_seq // 2
    n_tok = x_hbm.shape[0]
    n_chunks = n_tok // CHUNK
    n_q = wa_ref.shape[1] // COLS
    pieces = sloc.shape[0]
    halo_rows = pl.ds(0, HALO)

    def tail_copy(target):
        return pltpu.make_async_remote_copy(
            src_ref=tail_ref, dst_ref=xext.at[halo_rows], send_sem=misc.at[1], recv_sem=misc.at[2],
            device_id={'sp': target}, device_id_type=MESH)

    def decay_copy(target):
        return pltpu.make_async_remote_copy(
            src_ref=dall_ref, dst_ref=dpart, send_sem=misc.at[3], recv_sem=misc.at[4],
            device_id={'sp': target}, device_id_type=MESH)

    def state_copy(p, target):
        return pltpu.make_async_remote_copy(
            src_ref=sloc.at[p], dst_ref=s1buf.at[p], send_sem=send_a.at[p], recv_sem=recv_s.at[p],
            device_id={'sp': target}, device_id_type=MESH)

    def entry_copy(p, target):
        return pltpu.make_async_remote_copy(
            src_ref=sloc.at[p], dst_ref=rbuf.at[p], send_sem=send_a.at[p], recv_sem=recv_r.at[p],
            device_id={'sp': target}, device_id_type=MESH)

    def chain_copy(p, target):
        return pltpu.make_async_remote_copy(
            src_ref=s1buf.at[p], dst_ref=rbuf.at[p], send_sem=send_b.at[p], recv_sem=recv_r.at[p],
            device_id={'sp': target}, device_id_type=MESH)

    def out_copy(p):
        return pltpu.make_async_copy(rbuf.at[p], sin_hbm.at[p], out_sem.at[p])

    @pl.when(j == 0)
    def _():
        own = pltpu.make_async_copy(x_hbm, xext.at[pl.ds(HALO, n_tok)], misc.at[0])
        own.start()
        barrier = pltpu.get_barrier_semaphore()
        links = [(idx > 0, idx - 1), (idx < n_seq - 1, idx + 1),
                 ((core == 0) & (idx > 1), idx - 2), ((core == 0) & (idx < n_seq - 2), idx + 2)]
        for ok, other in links:
            @pl.when(ok)
            def _(other=other):
                pl.semaphore_signal(barrier, inc=1, device_id={'sp': other}, device_id_type=MESH)
        pl.semaphore_wait(barrier, sum(ok.astype(jnp.int32) for ok, other in links))

        @pl.when(idx < n_seq - 1)
        def _():
            tail_copy(idx + 1).start()

        @pl.when(core == 1)
        def _():
            decay_copy(idx - 1).start()

        @pl.when(idx == 0)
        def _():
            xext[halo_rows, :] = jnp.zeros((HALO, xext.shape[1]), BF16)

            def clear(p, carry):
                rbuf[p] = jnp.zeros(rbuf.shape[1:], F32)
                return carry
            lax.fori_loop(0, pieces, clear, 0)

        @pl.when(idx > 0)
        def _():
            tail_copy(idx).wait_recv()
        own.wait()

    def tick(t):
        @pl.when((core == 1) & (t < pieces))
        def _():
            state_copy(t, idx - 1).start()

        p = t - 1 - LAG * chip

        @pl.when((core == 0) & (p >= 0) & (p < pieces))
        def _():
            @pl.when(p == 0)
            def _():
                decay_copy(idx).wait_recv()
            state_copy(p, idx).wait_recv()

            @pl.when(chip > 0)
            def _():
                entry_copy(p, idx).wait_recv()
            grp = lax.div(p, n_q)
            lanes = pl.ds(pl.multiple_of(lax.rem(p, n_q) * COLS, COLS), COLS)
            d_own = dall_ref[pl.ds(grp, 1), lanes]
            d_par = dpart[pl.ds(grp, 1), lanes]
            mid = d_own * rbuf[p] + sloc[p]
            sloc[p] = mid
            s1buf[p] = d_par * mid + s1buf[p]

            @pl.when(chip < n_chip - 1)
            def _():
                chain_copy(p, idx + 2).start()
            entry_copy(p, idx + 1).start()
            out_copy(p).start()

        r = p - 2

        @pl.when((core == 1) & (r >= 0) & (r < pieces))
        def _():
            entry_copy(r, idx).wait_recv()
            out_copy(r).start()

    def conv(cw_ref, cb_ref, lanes):
        acc = cb_ref[0:1, lanes] + cw_ref[0:1, lanes] * pbuf[pl.ds(HALO, n_tok), :]
        for k in range(1, 4):
            m = mask_ref[k - 1]
            m = jnp.concatenate([m] * (COLS // m.shape[1]), axis=1)
            acc = acc + cw_ref[k:k + 1, lanes] * (m * pbuf[pl.ds(HALO - k, n_tok), :])
        half = 0.5 * acc
        return (half + half * jnp.tanh(half)).astype(BF16)

    def project(w):
        pbuf[...] = dot(xext[...], w).astype(BF16).astype(F32)

    def lane_block(q):
        return pl.ds(pl.multiple_of(q * COLS, COLS), COLS)

    @pl.when(j < groups)
    def _():
        par = lax.rem(j, 2)

        def epi_bc():
            v = conv(cwb_ref, cbb_ref, slice(0, COLS))
            bco_ref[...] = v
            half = COLS // 2
            vt = v.T
            btbuf[2 * par] = vt[:half]
            btbuf[2 * par + 1] = vt[half:]

        def epi_x(q):
            lanes = lane_block(q)
            v = conv(cwx_ref, cbx_ref, lanes)
            xo_ref[:, lanes] = v
            wexp = dot(wend_ref[0], e_ref[:, lanes])
            xs = (v.astype(F32) * wexp).astype(BF16)
            tot = None
            for c in range(n_chunks):
                st = dot(btbuf[par, :, c * CHUNK:(c + 1) * CHUNK], xs[c * CHUNK:(c + 1) * CHUNK])
                if c == 0:
                    st0_ref[0, :, lanes] = st
                    tot = st
                else:
                    tot = eexp_ref[0, c:c + 1, lanes] * tot + st
            sloc[j * n_q + q] = tot

        project(wbc_ref[...])
        epi_bc()
        project(wa_ref[:, 0:COLS])

        def body(q, carry):
            epi_x(q)
            project(wa_ref[:, lane_block(q + 1)])
            tick(j * n_q + q)
            return carry
        lax.fori_loop(0, n_q - 1, body, 0)
        epi_x(n_q - 1)
        tick(j * n_q + n_q - 1)

    @pl.when(j >= groups)
    def _():
        def body(q, carry):
            lanes = lane_block(q)
            z_ref[:, lanes] = dot(xext[pl.ds(HALO, n_tok), :], wa_ref[:, lanes]).astype(BF16)
            tick(j * n_q + q)
            return carry
        lax.fori_loop(0, n_q, body, 0)

    @pl.when(j == 2 * groups - 1)
    def _():
        @pl.when(idx < n_seq - 1)
        def _():
            tail_copy(idx).wait_send()

        @pl.when(core == 1)
        def _():
            decay_copy(idx).wait_send()

        def drain(p, carry):
            state_copy(p, idx).wait_send()

            @pl.when((core == 0) & (chip < n_chip - 1))
            def _():
                chain_copy(p, idx).wait_send()
            out_copy(p).wait()
            return carry
        lax.fori_loop(0, pieces, drain, 0)


def finish_kernel(per, head, x_ref, z_ref, b_ref, c_ref, ai_ref, ajt_ref, wst_ref, segc_ref, segr_ref,
                  sin_ref, st0_ref, eexp_ref, e_ref, norm_ref, w_ref, o_ref, sc_ref, y_ref, g_ref, acc_ref):
    i = pl.program_id(0)
    groups = norm_ref.shape[0]
    n_tok, width = x_ref.shape
    n_heads = ai_ref.shape[1]
    n_chunks = n_tok // CHUNK
    half = CHUNK // 2
    pair = 2 * head
    n_q = width // COLS
    out_cols = w_ref.shape[1] // n_q

    def masked_scores():
        row = lax.broadcasted_iota(jnp.int32, (CHUNK, CHUNK), 0)
        col = lax.broadcasted_iota(jnp.int32, (CHUNK, CHUNK), 1)
        for c in range(n_chunks):
            rows = slice(c * CHUNK, (c + 1) * CHUNK)
            raw = dot_nt(c_ref[rows, :], b_ref[rows, :])
            sc = segc_ref[rows, :]
            sc = jnp.concatenate([sc] * (CHUNK // sc.shape[1]), axis=1)
            same = sc == segr_ref[0:1, rows]
            sc_ref[c] = jnp.where(same & (row >= col), raw, 0.0)

    def mix_quad(q):
        first = lax.broadcasted_iota(jnp.int32, (half, pair), 1) < head
        lanes = pl.ds(pl.multiple_of(q * COLS, COLS), COLS)
        per_q = COLS // head
        ai = pltpu.roll(ai_ref[...], lax.rem(n_heads - (i * per + q * per_q), n_heads), 1)
        for c in range(n_chunks):
            r0 = c * CHUNK
            rows = slice(r0, r0 + CHUNK)
            sc = sc_ref.at[c]
            state = sin_ref[q]
            if c > 0:
                state = eexp_ref[0, 0:1, lanes] * state + st0_ref[0, :, lanes]
            ys = dot(c_ref[rows, :], state.astype(BF16)) * dot(wst_ref[0, rows, :], e_ref[:, lanes])
            y_ref[rows, lanes] = ys + eexp_ref[0, 7:8, lanes] * x_ref[rows, lanes].astype(F32)
            for hp in range(per_q // 2):
                pl_lanes = pl.ds(pl.multiple_of(q * COLS + hp * pair, pair), pair)
                xp = x_ref[rows, pl_lanes]
                tops, bots = [], []
                for hh in range(2):
                    k = 2 * hp + hh
                    aj = ajt_ref[pl.ds(q * per_q + k, 1), rows]
                    ai_t = ai[r0:r0 + half, k:k + 1]
                    ai_b = ai[r0 + half:r0 + CHUNK, k:k + 1]
                    m_tt = sc[0:half, 0:half] * jnp.exp2(jnp.minimum(ai_t - aj[:, 0:half], 127.99))
                    m_bl = sc[half:CHUNK, 0:half] * jnp.exp2(jnp.minimum(ai_b - aj[:, 0:half], 127.99))
                    m_br = sc[half:CHUNK, half:CHUNK] * jnp.exp2(jnp.minimum(ai_b - aj[:, half:CHUNK], 127.99))
                    tops.append(dot(m_tt.astype(BF16), xp[0:half]))
                    m_b = jnp.concatenate([m_bl.astype(BF16), m_br.astype(BF16)], axis=1)
                    bots.append(dot(m_b, xp))
                for top, parts in ((r0, tops), (r0 + half, bots)):
                    sub = slice(top, top + half)
                    y = y_ref[sub, pl_lanes] + jnp.where(first, parts[0], parts[1])
                    hz = 0.5 * z_ref[sub, pl_lanes].astype(F32)
                    y_ref[sub, pl_lanes] = y * (hz + hz * jnp.tanh(hz))

    def normalize():
        y = y_ref[...]
        mean = jnp.sum(y * y, axis=1, keepdims=True) * (1.0 / width)
        g_ref[...] = (y * lax.rsqrt(mean + EPS) * norm_ref[pl.ds(i, 1), :]).astype(BF16)

    def out_part(q):
        cols = pl.ds(pl.multiple_of(q * out_cols, out_cols), out_cols)
        acc_ref[:, cols] += dot(g_ref[...], w_ref[:, cols])

    @pl.when(i == 0)
    def _():
        masked_scores()

        def body(q, carry):
            cols = pl.ds(pl.multiple_of(q * out_cols, out_cols), out_cols)
            acc_ref[:, cols] = jnp.zeros((n_tok, out_cols), F32)
            mix_quad(q)
            return carry
        lax.fori_loop(0, n_q, body, 0)
        normalize()

    @pl.when((i > 0) & (i < groups))
    def _():
        masked_scores()

        def body(q, carry):
            out_part(q)
            mix_quad(q)
            return carry
        lax.fori_loop(0, n_q, body, 0)
        normalize()

    @pl.when(i == groups)
    def _():
        def body(q, carry):
            cols = pl.ds(pl.multiple_of(q * out_cols, out_cols), out_cols)
            o_ref[:, cols] = (acc_ref[:, cols] + dot(g_ref[...], w_ref[:, cols])).astype(BF16)
            return carry
        lax.fori_loop(0, n_q, body, 0)


def solution(mesh):
    n_seq = mesh.shape['sp']
    row_spec = P(('dp', 'sp'), None)
    tok_spec = P(('dp', 'sp'))

    def layer_shard(x, doc_start, w_in, conv_w, conv_b, dt_bias, a_log, d_skip, norm_w, w_out):
        n_tok, d_model = x.shape
        groups, gw = norm_w.shape
        d_inner = groups * gw
        n_heads = a_log.shape[0]
        per = n_heads // groups
        head = d_inner // n_heads
        conv_dim = conv_w.shape[1]
        sdim = (conv_dim - d_inner) // (2 * groups)
        n_q = gw // COLS
        n_chunks = n_tok // CHUNK
        pieces = groups * n_q
        lim = 67043328

        sds = jax.ShapeDtypeStruct
        full = lambda *shape: pl.BlockSpec(shape, lambda i: (0,) * len(shape))
        k3 = 3 * per
        dt_block = (d_inner + conv_dim) // n_heads
        prep = pl.pallas_call(
            functools.partial(prep_kernel, per, head),
            grid=(1,),
            in_specs=[full(n_tok, d_model), pl.BlockSpec((d_model, n_heads), lambda i: (0, dt_block)),
                      full(1, n_heads), full(1, n_heads), full(1, n_heads), full(1, n_tok)],
            out_specs=[full(n_tok, n_heads), full(n_heads, n_tok), full(groups, n_tok, k3), full(groups, n_tok, k3),
                       full(groups, 8, gw), full(groups, gw), full(3, n_tok, 128), full(HALO, d_model),
                       full(n_tok, 128), full(8, n_tok), full(k3, gw)],
            out_shape=[sds((n_tok, n_heads), F32), sds((n_heads, n_tok), F32), sds((groups, n_tok, k3), BF16),
                       sds((groups, n_tok, k3), BF16), sds((groups, 8, gw), F32), sds((groups, gw), F32),
                       sds((3, n_tok, 128), F32), sds((HALO, d_model), BF16), sds((n_tok, 128), F32), sds((8, n_tok), F32), sds((k3, gw), BF16)],
            scratch_shapes=[VMEM((n_tok + 8, 128), F32)],
            compiler_params=pltpu.CompilerParams(vmem_limit_bytes=lim),
            name='prep',
        )
        ai, ajt, wst3, wend3, eexp, dall, masks, tail, segc, segr, expand = prep(
            x, w_in, dt_bias[None], a_log[None], d_skip[None], doc_start[None])

        cap = lambda i: jnp.minimum(i, groups - 1)
        z_of = lambda i: jnp.maximum(i - groups, 0)
        pairs = groups // 2
        bc_of = lambda i: lax.rem(cap(i), 2) * pairs + lax.div(cap(i), 2)
        x_blk = d_inner // gw
        bc_blk = 2 * d_inner // COLS
        cb_blk = d_inner // COLS
        proj = pl.pallas_call(
            functools.partial(proj_kernel, n_seq, groups),
            grid=(2 * groups,),
            in_specs=[pl.BlockSpec(memory_space=pl.ANY), full(HALO, d_model),
                      pl.BlockSpec((d_model, gw), lambda i: (0, jnp.where(i < groups, i + x_blk, i - groups))),
                      pl.BlockSpec((d_model, COLS), lambda i: (0, bc_blk + bc_of(i))),
                      pl.BlockSpec((4, gw), lambda i: (0, cap(i))), pl.BlockSpec((1, gw), lambda i: (0, cap(i))),
                      pl.BlockSpec((4, COLS), lambda i: (0, cb_blk + bc_of(i))), pl.BlockSpec((1, COLS), lambda i: (0, cb_blk + bc_of(i))),
                      full(3, n_tok, 128),
                      pl.BlockSpec((1, n_tok, k3), lambda i: (cap(i), 0, 0)),
                      pl.BlockSpec((1, 8, gw), lambda i: (cap(i), 0, 0)),
                      full(groups, gw), full(k3, gw)],
            out_specs=[pl.BlockSpec((n_tok, gw), lambda i: (0, cap(i))),
                       pl.BlockSpec((n_tok, COLS), lambda i: (0, bc_of(i))),
                       pl.BlockSpec((n_tok, gw), lambda i: (0, z_of(i))),
                       pl.BlockSpec((1, sdim, gw), lambda i: (cap(i), 0, 0)),
                       pl.BlockSpec(memory_space=pl.ANY)],
            out_shape=[sds((n_tok, d_inner), BF16), sds((n_tok, conv_dim - d_inner), BF16), sds((n_tok, d_inner), BF16),
                       sds((groups, sdim, gw), F32), sds((pieces, sdim, COLS), F32)],
            scratch_shapes=[VMEM((n_tok + HALO, d_model), BF16), VMEM((n_tok + HALO, COLS), F32),
                            VMEM((4, sdim, n_tok), BF16), VMEM((pieces, sdim, COLS), F32),
                            VMEM((pieces, sdim, COLS), F32), VMEM((pieces, sdim, COLS), F32), VMEM((groups, gw), F32),
                            pltpu.SemaphoreType.DMA((pieces,)), pltpu.SemaphoreType.DMA((pieces,)),
                            pltpu.SemaphoreType.DMA((pieces,)), pltpu.SemaphoreType.DMA((pieces,)),
                            pltpu.SemaphoreType.DMA((pieces,)), pltpu.SemaphoreType.DMA((5,))],
            compiler_params=pltpu.CompilerParams(vmem_limit_bytes=lim, collective_id=0, has_side_effects=True),
            name='proj',
        )
        xc, bc, z, st0, s_in = proj(x, tail, w_in, w_in, conv_w, conv_b[None], conv_w, conv_b[None], masks, wend3, eexp, dall, expand)

        prev = lambda i: jnp.maximum(i - 1, 0)
        finish = pl.pallas_call(
            functools.partial(finish_kernel, per, head),
            grid=(groups + 1,),
            in_specs=[pl.BlockSpec((n_tok, gw), lambda i: (0, cap(i))), pl.BlockSpec((n_tok, gw), lambda i: (0, cap(i))),
                      pl.BlockSpec((n_tok, sdim), lambda i: (0, cap(i))), pl.BlockSpec((n_tok, sdim), lambda i: (0, groups + cap(i))),
                      full(n_tok, n_heads), pl.BlockSpec((per, n_tok), lambda i: (cap(i), 0)),
                      pl.BlockSpec((1, n_tok, k3), lambda i: (cap(i), 0, 0)), full(n_tok, 128), full(8, n_tok),
                      pl.BlockSpec((n_q, sdim, COLS), lambda i: (cap(i), 0, 0)), pl.BlockSpec((1, sdim, gw), lambda i: (cap(i), 0, 0)),
                      pl.BlockSpec((1, 8, gw), lambda i: (cap(i), 0, 0)), full(k3, gw), full(groups, gw),
                      pl.BlockSpec((gw, d_model), lambda i: (prev(i), 0))],
            out_specs=full(n_tok, d_model),
            out_shape=sds((n_tok, d_model), BF16),
            scratch_shapes=[VMEM((n_chunks, CHUNK, CHUNK), F32), VMEM((n_tok, gw), F32), VMEM((n_tok, gw), BF16),
                            VMEM((n_tok, d_model), F32)],
            compiler_params=pltpu.CompilerParams(vmem_limit_bytes=lim),
            name='finish',
        )
        return finish(xc, z, bc, bc, ai, ajt, wst3, segc, segr, s_in, st0, eexp, expand, norm_w, w_out)

    return jax.shard_map(layer_shard, mesh=mesh, in_specs=(row_spec, tok_spec, P(), P(), P(), P(), P(), P(), P(), P()), out_specs=row_spec, check_vma=False)
```

```python
import functools
import jax
import jax.numpy as jnp
from jax import lax
from jax.experimental import pallas as pl
from jax.experimental.pallas import tpu as pltpu
from jax.sharding import PartitionSpec as P

CHUNK = 256
EPS = 1e-5
LOG2E = 1.4426950408889634
HALO = 16
COLS = 512
BC_COLS = 256
QUAD = 512
LAG = 2
LAG_BACK = 1
VMEM = pltpu.VMEM
MESH = pl.DeviceIdType.MESH
F32 = jnp.float32
BF16 = jnp.bfloat16


def split3(v):
    hi = v.astype(BF16)
    rest = v - hi.astype(F32)
    mid = rest.astype(BF16)
    lo = (rest - mid.astype(F32)).astype(BF16)
    return hi, mid, lo


def dot(a, b):
    return jnp.dot(a, b, preferred_element_type=F32)


def dot_nt(a, b):
    return lax.dot_general(a, b, (((1,), (1,)), ((), ())), preferred_element_type=F32)


def prep_kernel(per, head, x_ref, w_ref, bias_ref, alog_ref, skip_ref, doc_ref,
                ai_ref, ajt_ref, wst_ref, wend_ref, eexp_ref, dall_ref, mask_ref,
                tail_ref, segc_ref, segr_ref, e_ref, keep_ref):
    n_tok = x_ref.shape[0]
    doc = doc_ref[...].astype(F32)
    docr = jnp.broadcast_to(doc, (8, n_tok)).astype(BF16)
    docf = jnp.broadcast_to(doc, (128, n_tok)).T
    docc = docf.astype(BF16)
    e_row = lax.rem(lax.broadcasted_iota(jnp.int32, e_ref.shape, 0), per)
    e_col = lax.div(lax.broadcasted_iota(jnp.int32, e_ref.shape, 1), head)
    expand = (e_row == e_col).astype(F32).astype(BF16)
    e_ref[...] = expand
    groups = wst_ref.shape[0]
    n_chunks = n_tok // CHUNK
    raw = dot(x_ref[...], w_ref[...]).astype(BF16).astype(F32) + bias_ref[...]
    dt = jnp.maximum(raw, 0.0) + jnp.log1p(jnp.exp(-jnp.abs(raw)))
    a = -jnp.exp(alog_ref[...]) * dt
    row = lax.broadcasted_iota(jnp.int32, (CHUNK, CHUNK), 0)
    col = lax.broadcasted_iota(jnp.int32, (CHUNK, CHUNK), 1)
    tri = (row >= col).astype(F32).astype(BF16)
    last_rows = []
    for c in range(n_chunks):
        rows = pl.ds(c * CHUNK, CHUNK)
        sl = slice(c * CHUNK, (c + 1) * CHUNK)
        hi, mid, lo = split3(a[sl])
        acum = dot(tri, hi) + (dot(tri, mid) + dot(tri, lo))
        dtc = dt[sl]
        segc = dot(tri, docc[sl])
        segc_ref[rows, :] = segc
        segr_ref[:, rows] = dot_nt(docr[:, sl], tri)
        a_last = acum[CHUNK - 1:CHUNK]
        s_last = segc[CHUNK - 1:CHUNK]
        wend = jnp.where(segc == s_last, jnp.exp(a_last - acum) * dtc, 0.0)
        wst = jnp.where(segc == 0.0, jnp.exp(acum), 0.0)
        e_c = jnp.where(s_last == 0.0, jnp.exp(a_last), 0.0)
        last_rows.append(e_c)
        ai = acum * LOG2E
        ai_ref[rows, :] = ai
        ajt_ref[:, rows] = (ai - jnp.log2(dtc)).T
        end3 = split3(wend)
        st3 = split3(wst)
        for g in range(groups):
            lanes = slice(g * per, (g + 1) * per)
            wend_ref[g, rows, :] = jnp.concatenate([v[:, lanes] for v in end3], axis=1)
            wst_ref[g, rows, :] = jnp.concatenate([v[:, lanes] for v in st3], axis=1)
    total = last_rows[0]
    for e_c in last_rows[1:]:
        total = total * e_c
    n_row = len(last_rows)
    stack = jnp.concatenate(last_rows + [total] * (7 - n_row) + [skip_ref[...]], axis=0)
    parts = split3(stack)
    for g in range(groups):
        lanes = slice(g * per, (g + 1) * per)
        cat = jnp.concatenate([v[:, lanes] for v in parts], axis=1)
        ex = dot(cat, expand)
        eexp_ref[g] = ex
        dall_ref[pl.ds(g, 1), :] = ex[n_row:n_row + 1]
    keep_ref[pl.ds(0, 8), :] = jnp.ones((8, docf.shape[1]), F32)
    keep_ref[pl.ds(8, n_tok), :] = 1.0 - docf
    m1 = keep_ref[pl.ds(8, n_tok), :]
    m2 = m1 * keep_ref[pl.ds(7, n_tok), :]
    m3 = m2 * keep_ref[pl.ds(6, n_tok), :]
    mask_ref[0] = m1
    mask_ref[1] = m2
    mask_ref[2] = m3
    r16 = lax.broadcasted_iota(jnp.int32, (HALO, HALO), 0)
    c16 = lax.broadcasted_iota(jnp.int32, (HALO, HALO), 1)
    later = (c16 > r16).astype(F32).astype(BF16)
    cnt = dot(later, docc[n_tok - HALO:])
    tail = x_ref[pl.ds(n_tok - HALO, HALO), :].astype(F32)
    tail_ref[...] = jnp.where(cnt[:, :1] == 0.0, tail, 0.0).astype(BF16)


def proj_kernel(n_seq, groups, x_hbm, tail_ref, wa_ref, wbc_ref, cwx_ref, cbx_ref, cwb_ref, cbb_ref,
                mask_ref, wend_ref, eexp_ref, dall_ref, e_ref,
                xo_ref, bco_ref, z_ref, st0_ref, sin_hbm,
                xext, pbuf, bbuf, btbuf, sloc, s1buf, rbuf, dpart,
                send_a, send_b, recv_s, recv_r, out_sem, misc):
    j = pl.program_id(0)
    idx = lax.axis_index('sp')
    core = lax.rem(idx, 2)
    chip = lax.div(idx, 2)
    n_chip = n_seq // 2
    n_tok = x_hbm.shape[0]
    n_chunks = n_tok // CHUNK
    n_q = wa_ref.shape[1] // COLS
    pieces = sloc.shape[0]
    halo_rows = pl.ds(0, HALO)

    def tail_copy(target):
        return pltpu.make_async_remote_copy(
            src_ref=tail_ref, dst_ref=xext.at[halo_rows], send_sem=misc.at[1], recv_sem=misc.at[2],
            device_id={'sp': target}, device_id_type=MESH)

    def decay_copy(target):
        return pltpu.make_async_remote_copy(
            src_ref=dall_ref, dst_ref=dpart, send_sem=misc.at[3], recv_sem=misc.at[4],
            device_id={'sp': target}, device_id_type=MESH)

    def state_copy(p, target):
        return pltpu.make_async_remote_copy(
            src_ref=sloc.at[p], dst_ref=s1buf.at[p], send_sem=send_a.at[p], recv_sem=recv_s.at[p],
            device_id={'sp': target}, device_id_type=MESH)

    def entry_copy(p, target):
        return pltpu.make_async_remote_copy(
            src_ref=sloc.at[p], dst_ref=rbuf.at[p], send_sem=send_a.at[p], recv_sem=recv_r.at[p],
            device_id={'sp': target}, device_id_type=MESH)

    def chain_copy(p, target):
        return pltpu.make_async_remote_copy(
            src_ref=s1buf.at[p], dst_ref=rbuf.at[p], send_sem=send_b.at[p], recv_sem=recv_r.at[p],
            device_id={'sp': target}, device_id_type=MESH)

    def out_copy(p):
        return pltpu.make_async_copy(rbuf.at[p], sin_hbm.at[p], out_sem.at[p])

    @pl.when(j == 0)
    def _():
        own = pltpu.make_async_copy(x_hbm, xext.at[pl.ds(HALO, n_tok)], misc.at[0])
        own.start()
        barrier = pltpu.get_barrier_semaphore()
        links = [(idx > 0, idx - 1), (idx < n_seq - 1, idx + 1),
                 ((core == 0) & (idx > 1), idx - 2), ((core == 0) & (idx < n_seq - 2), idx + 2)]
        for ok, other in links:
            @pl.when(ok)
            def _(other=other):
                pl.semaphore_signal(barrier, inc=1, device_id={'sp': other}, device_id_type=MESH)
        pl.semaphore_wait(barrier, sum(ok.astype(jnp.int32) for ok, other in links))

        @pl.when(idx < n_seq - 1)
        def _():
            tail_copy(idx + 1).start()

        @pl.when(core == 1)
        def _():
            decay_copy(idx - 1).start()

        @pl.when(idx == 0)
        def _():
            xext[halo_rows, :] = jnp.zeros((HALO, xext.shape[1]), BF16)

            def clear(p, carry):
                rbuf[p] = jnp.zeros(rbuf.shape[1:], F32)
                return carry
            lax.fori_loop(0, pieces, clear, 0)

        @pl.when(idx > 0)
        def _():
            tail_copy(idx).wait_recv()
        own.wait()

    def tick(t):
        @pl.when((core == 1) & (t < pieces))
        def _():
            state_copy(t, idx - 1).start()

        p = t - 1 - LAG * chip

        @pl.when((core == 0) & (p >= 0) & (p < pieces))
        def _():
            @pl.when(p == 0)
            def _():
                decay_copy(idx).wait_recv()
            state_copy(p, idx).wait_recv()

            @pl.when(chip > 0)
            def _():
                entry_copy(p, idx).wait_recv()
            grp = lax.div(p, n_q)
            lanes = pl.ds(pl.multiple_of(lax.rem(p, n_q) * COLS, COLS), COLS)
            d_own = dall_ref[pl.ds(grp, 1), lanes]
            d_par = dpart[pl.ds(grp, 1), lanes]
            mid = d_own * rbuf[p] + sloc[p]
            sloc[p] = mid
            s1buf[p] = d_par * mid + s1buf[p]

            @pl.when(chip < n_chip - 1)
            def _():
                chain_copy(p, idx + 2).start()
            entry_copy(p, idx + 1).start()
            out_copy(p).start()

        r = p - LAG_BACK

        @pl.when((core == 1) & (r >= 0) & (r < pieces))
        def _():
            entry_copy(r, idx).wait_recv()
            out_copy(r).start()

    def conv(buf, cw_ref, cb_ref, lanes):
        cols = buf.shape[1]
        acc = cb_ref[0:1, lanes] + cw_ref[0:1, lanes] * buf[pl.ds(HALO, n_tok), :]
        for k in range(1, 4):
            m = mask_ref[k - 1]
            m = jnp.concatenate([m] * (cols // m.shape[1]), axis=1)
            acc = acc + cw_ref[k:k + 1, lanes] * (m * buf[pl.ds(HALO - k, n_tok), :])
        half = 0.5 * acc
        return (half + half * jnp.tanh(half)).astype(BF16)

    def project(buf, w):
        buf[...] = dot(xext[...], w).astype(BF16).astype(F32)

    @pl.when(j < groups)
    def _():
        par = lax.rem(j, 2)

        def epi_bc():
            v = conv(bbuf, cwb_ref, cbb_ref, slice(0, BC_COLS))
            bco_ref[...] = v
            half = BC_COLS // 2
            vt = v.T
            btbuf[2 * par] = vt[:half]
            btbuf[2 * par + 1] = vt[half:]

        def epi_x(q, buf):
            lanes = slice(q * COLS, (q + 1) * COLS)
            v = conv(buf, cwx_ref, cbx_ref, lanes)
            xo_ref[:, lanes] = v
            wexp = dot(wend_ref[0], e_ref[:, lanes])
            xs = (v.astype(F32) * wexp).astype(BF16)
            tot = None
            for c in range(n_chunks):
                st = dot(btbuf[par, :, c * CHUNK:(c + 1) * CHUNK], xs[c * CHUNK:(c + 1) * CHUNK])
                if c == 0:
                    st0_ref[0, :, lanes] = st
                    tot = st
                else:
                    tot = eexp_ref[0, c:c + 1, lanes] * tot + st
            sloc[j * n_q + q] = tot

        project(bbuf, wbc_ref[...])
        project(pbuf.at[0], wa_ref[:, 0:COLS])
        epi_bc()
        for q in range(n_q - 1):
            project(pbuf.at[(q + 1) % 2], wa_ref[:, (q + 1) * COLS:(q + 2) * COLS])
            epi_x(q, pbuf.at[q % 2])
            tick(j * n_q + q)
        epi_x(n_q - 1, pbuf.at[(n_q - 1) % 2])
        tick(j * n_q + n_q - 1)

    @pl.when(j >= groups)
    def _():
        def body(q, carry):
            lanes = pl.ds(pl.multiple_of(q * COLS, COLS), COLS)
            z_ref[:, lanes] = dot(xext[pl.ds(HALO, n_tok), :], wa_ref[:, lanes]).astype(BF16)
            tick(j * n_q + q)
            return carry
        lax.fori_loop(0, n_q, body, 0)

    @pl.when(j == 2 * groups - 1)
    def _():
        @pl.when(idx < n_seq - 1)
        def _():
            tail_copy(idx).wait_send()

        @pl.when(core == 1)
        def _():
            decay_copy(idx).wait_send()

        def drain(p, carry):
            state_copy(p, idx).wait_send()

            @pl.when((core == 0) & (chip < n_chip - 1))
            def _():
                chain_copy(p, idx).wait_send()
            out_copy(p).wait()
            return carry
        lax.fori_loop(0, pieces, drain, 0)


def finish_kernel(per, head, x_ref, z_ref, b_ref, c_ref, ai_ref, ajt_ref, wst_ref, segc_ref, segr_ref,
                  sin_ref, st0_ref, eexp_ref, e_ref, norm_ref, w_ref, o_ref, sc_ref, y_ref, g_ref, acc_ref):
    i = pl.program_id(0)
    groups = norm_ref.shape[0]
    n_tok, width = x_ref.shape
    n_heads = ai_ref.shape[1]
    n_chunks = n_tok // CHUNK
    half = CHUNK // 2
    pair = 2 * head
    n_q = width // QUAD
    n_sub = sin_ref.shape[2] // QUAD
    out_cols = w_ref.shape[1] // n_q

    def masked_scores():
        row = lax.broadcasted_iota(jnp.int32, (CHUNK, CHUNK), 0)
        col = lax.broadcasted_iota(jnp.int32, (CHUNK, CHUNK), 1)
        for c in range(n_chunks):
            rows = slice(c * CHUNK, (c + 1) * CHUNK)
            raw = dot_nt(c_ref[rows, :], b_ref[rows, :])
            sc = segc_ref[rows, :]
            sc = jnp.concatenate([sc] * (CHUNK // sc.shape[1]), axis=1)
            same = sc == segr_ref[0:1, rows]
            sc_ref[c] = jnp.where(same & (row >= col), raw, 0.0)

    def mix_quad(q):
        first = lax.broadcasted_iota(jnp.int32, (half, pair), 1) < head
        lanes = pl.ds(pl.multiple_of(q * QUAD, QUAD), QUAD)
        per_q = QUAD // head
        ai = pltpu.roll(ai_ref[...], lax.rem(n_heads - (i * per + q * per_q), n_heads), 1)
        for c in range(n_chunks):
            r0 = c * CHUNK
            rows = slice(r0, r0 + CHUNK)
            sc = sc_ref.at[c]
            state = sin_ref[lax.div(q, n_sub), :, pl.ds(pl.multiple_of(lax.rem(q, n_sub) * QUAD, QUAD), QUAD)]
            if c > 0:
                state = eexp_ref[0, 0:1, lanes] * state + st0_ref[0, :, lanes]
            ys = dot(c_ref[rows, :], state.astype(BF16)) * dot(wst_ref[0, rows, :], e_ref[:, lanes])
            y_ref[rows, lanes] = ys + eexp_ref[0, 7:8, lanes] * x_ref[rows, lanes].astype(F32)
            for hp in range(per_q // 2):
                pl_lanes = pl.ds(pl.multiple_of(q * QUAD + hp * pair, pair), pair)
                xp = x_ref[rows, pl_lanes]
                tops, bots = [], []
                for hh in range(2):
                    k = 2 * hp + hh
                    aj = ajt_ref[pl.ds(q * per_q + k, 1), rows]
                    ai_t = ai[r0:r0 + half, k:k + 1]
                    ai_b = ai[r0 + half:r0 + CHUNK, k:k + 1]
                    m_tt = sc[0:half, 0:half] * jnp.exp2(jnp.minimum(ai_t - aj[:, 0:half], 127.99))
                    m_bl = sc[half:CHUNK, 0:half] * jnp.exp2(jnp.minimum(ai_b - aj[:, 0:half], 127.99))
                    m_br = sc[half:CHUNK, half:CHUNK] * jnp.exp2(jnp.minimum(ai_b - aj[:, half:CHUNK], 127.99))
                    tops.append(dot(m_tt.astype(BF16), xp[0:half]))
                    m_b = jnp.concatenate([m_bl.astype(BF16), m_br.astype(BF16)], axis=1)
                    bots.append(dot(m_b, xp))
                for top, parts in ((r0, tops), (r0 + half, bots)):
                    sub = slice(top, top + half)
                    y = y_ref[sub, pl_lanes] + jnp.where(first, parts[0], parts[1])
                    hz = 0.5 * z_ref[sub, pl_lanes].astype(F32)
                    y_ref[sub, pl_lanes] = y * (hz + hz * jnp.tanh(hz))

    def normalize():
        y = y_ref[...]
        mean = jnp.sum(y * y, axis=1, keepdims=True) * (1.0 / width)
        g_ref[...] = (y * lax.rsqrt(mean + EPS) * norm_ref[pl.ds(i, 1), :]).astype(BF16)

    def out_part(q):
        cols = pl.ds(pl.multiple_of(q * out_cols, out_cols), out_cols)
        acc_ref[:, cols] += dot(g_ref[...], w_ref[:, cols])

    @pl.when(i == 0)
    def _():
        masked_scores()

        def body(q, carry):
            cols = pl.ds(pl.multiple_of(q * out_cols, out_cols), out_cols)
            acc_ref[:, cols] = jnp.zeros((n_tok, out_cols), F32)
            mix_quad(q)
            return carry
        lax.fori_loop(0, n_q, body, 0)
        normalize()

    @pl.when((i > 0) & (i < groups))
    def _():
        masked_scores()

        def body(q, carry):
            out_part(q)
            mix_quad(q)
            return carry
        lax.fori_loop(0, n_q, body, 0)
        normalize()

    @pl.when(i == groups)
    def _():
        def body(q, carry):
            cols = pl.ds(pl.multiple_of(q * out_cols, out_cols), out_cols)
            o_ref[:, cols] = (acc_ref[:, cols] + dot(g_ref[...], w_ref[:, cols])).astype(BF16)
            return carry
        lax.fori_loop(0, n_q, body, 0)


def solution(mesh):
    n_seq = mesh.shape['sp']
    row_spec = P(('dp', 'sp'), None)
    tok_spec = P(('dp', 'sp'))

    def layer_shard(x, doc_start, w_in, conv_w, conv_b, dt_bias, a_log, d_skip, norm_w, w_out):
        n_tok, d_model = x.shape
        groups, gw = norm_w.shape
        d_inner = groups * gw
        n_heads = a_log.shape[0]
        per = n_heads // groups
        head = d_inner // n_heads
        conv_dim = conv_w.shape[1]
        sdim = (conv_dim - d_inner) // (2 * groups)
        n_q = gw // COLS
        n_chunks = n_tok // CHUNK
        pieces = groups * n_q
        lim = 67043328

        sds = jax.ShapeDtypeStruct
        full = lambda *shape: pl.BlockSpec(shape, lambda i: (0,) * len(shape))
        k3 = 3 * per
        dt_block = (d_inner + conv_dim) // n_heads
        prep = pl.pallas_call(
            functools.partial(prep_kernel, per, head),
            grid=(1,),
            in_specs=[full(n_tok, d_model), pl.BlockSpec((d_model, n_heads), lambda i: (0, dt_block)),
                      full(1, n_heads), full(1, n_heads), full(1, n_heads), full(1, n_tok)],
            out_specs=[full(n_tok, n_heads), full(n_heads, n_tok), full(groups, n_tok, k3), full(groups, n_tok, k3),
                       full(groups, 8, gw), full(groups, gw), full(3, n_tok, 128), full(HALO, d_model),
                       full(n_tok, 128), full(8, n_tok), full(k3, gw)],
            out_shape=[sds((n_tok, n_heads), F32), sds((n_heads, n_tok), F32), sds((groups, n_tok, k3), BF16),
                       sds((groups, n_tok, k3), BF16), sds((groups, 8, gw), F32), sds((groups, gw), F32),
                       sds((3, n_tok, 128), F32), sds((HALO, d_model), BF16), sds((n_tok, 128), F32), sds((8, n_tok), F32), sds((k3, gw), BF16)],
            scratch_shapes=[VMEM((n_tok + 8, 128), F32)],
            compiler_params=pltpu.CompilerParams(vmem_limit_bytes=lim),
            name='prep',
        )
        ai, ajt, wst3, wend3, eexp, dall, masks, tail, segc, segr, expand = prep(
            x, w_in, dt_bias[None], a_log[None], d_skip[None], doc_start[None])

        cap = lambda i: jnp.minimum(i, groups - 1)
        z_of = lambda i: jnp.maximum(i - groups, 0)
        pairs = groups // 2
        bc_of = lambda i: lax.rem(cap(i), 2) * pairs + lax.div(cap(i), 2)
        x_blk = d_inner // gw
        bc_blk = 2 * d_inner // BC_COLS
        cb_blk = d_inner // BC_COLS
        proj = pl.pallas_call(
            functools.partial(proj_kernel, n_seq, groups),
            grid=(2 * groups,),
            in_specs=[pl.BlockSpec(memory_space=pl.ANY), full(HALO, d_model),
                      pl.BlockSpec((d_model, gw), lambda i: (0, jnp.where(i < groups, i + x_blk, i - groups))),
                      pl.BlockSpec((d_model, BC_COLS), lambda i: (0, bc_blk + bc_of(i))),
                      pl.BlockSpec((4, gw), lambda i: (0, cap(i))), pl.BlockSpec((1, gw), lambda i: (0, cap(i))),
                      pl.BlockSpec((4, BC_COLS), lambda i: (0, cb_blk + bc_of(i))), pl.BlockSpec((1, BC_COLS), lambda i: (0, cb_blk + bc_of(i))),
                      full(3, n_tok, 128),
                      pl.BlockSpec((1, n_tok, k3), lambda i: (cap(i), 0, 0)),
                      pl.BlockSpec((1, 8, gw), lambda i: (cap(i), 0, 0)),
                      full(groups, gw), full(k3, gw)],
            out_specs=[pl.BlockSpec((n_tok, gw), lambda i: (0, cap(i))),
                       pl.BlockSpec((n_tok, BC_COLS), lambda i: (0, bc_of(i))),
                       pl.BlockSpec((n_tok, gw), lambda i: (0, z_of(i))),
                       pl.BlockSpec((1, sdim, gw), lambda i: (cap(i), 0, 0)),
                       pl.BlockSpec(memory_space=pl.ANY)],
            out_shape=[sds((n_tok, d_inner), BF16), sds((n_tok, conv_dim - d_inner), BF16), sds((n_tok, d_inner), BF16),
                       sds((groups, sdim, gw), F32), sds((pieces, sdim, COLS), F32)],
            scratch_shapes=[VMEM((n_tok + HALO, d_model), BF16), VMEM((2, n_tok + HALO, COLS), F32), VMEM((n_tok + HALO, BC_COLS), F32),
                            VMEM((4, sdim, n_tok), BF16), VMEM((pieces, sdim, COLS), F32),
                            VMEM((pieces, sdim, COLS), F32), VMEM((pieces, sdim, COLS), F32), VMEM((groups, gw), F32),
                            pltpu.SemaphoreType.DMA((pieces,)), pltpu.SemaphoreType.DMA((pieces,)),
                            pltpu.SemaphoreType.DMA((pieces,)), pltpu.SemaphoreType.DMA((pieces,)),
                            pltpu.SemaphoreType.DMA((pieces,)), pltpu.SemaphoreType.DMA((5,))],
            compiler_params=pltpu.CompilerParams(vmem_limit_bytes=lim, collective_id=0, has_side_effects=True),
            name='proj',
        )
        xc, bc, z, st0, s_in = proj(x, tail, w_in, w_in, conv_w, conv_b[None], conv_w, conv_b[None], masks, wend3, eexp, dall, expand)

        prev = lambda i: jnp.maximum(i - 1, 0)
        finish = pl.pallas_call(
            functools.partial(finish_kernel, per, head),
            grid=(groups + 1,),
            in_specs=[pl.BlockSpec((n_tok, gw), lambda i: (0, cap(i))), pl.BlockSpec((n_tok, gw), lambda i: (0, cap(i))),
                      pl.BlockSpec((n_tok, sdim), lambda i: (0, cap(i))), pl.BlockSpec((n_tok, sdim), lambda i: (0, groups + cap(i))),
                      full(n_tok, n_heads), pl.BlockSpec((per, n_tok), lambda i: (cap(i), 0)),
                      pl.BlockSpec((1, n_tok, k3), lambda i: (cap(i), 0, 0)), full(n_tok, 128), full(8, n_tok),
                      pl.BlockSpec((n_q, sdim, COLS), lambda i: (cap(i), 0, 0)), pl.BlockSpec((1, sdim, gw), lambda i: (cap(i), 0, 0)),
                      pl.BlockSpec((1, 8, gw), lambda i: (cap(i), 0, 0)), full(k3, gw), full(groups, gw),
                      pl.BlockSpec((gw, d_model), lambda i: (prev(i), 0))],
            out_specs=full(n_tok, d_model),
            out_shape=sds((n_tok, d_model), BF16),
            scratch_shapes=[VMEM((n_chunks, CHUNK, CHUNK), F32), VMEM((n_tok, gw), F32), VMEM((n_tok, gw), BF16),
                            VMEM((n_tok, d_model), F32)],
            compiler_params=pltpu.CompilerParams(vmem_limit_bytes=lim),
            name='finish',
        )
        return finish(xc, z, bc, bc, ai, ajt, wst3, segc, segr, s_in, st0, eexp, expand, norm_w, w_out)

    return jax.shard_map(layer_shard, mesh=mesh, in_specs=(row_spec, tok_spec, P(), P(), P(), P(), P(), P(), P(), P()), out_specs=row_spec, check_vma=False)
```
